512 devices in a mesh: leaf: 128 (over z, y, core), rhs: 4 (over x).
Axes of the slice: x: 4, y: 8, z: 8, core: 2. Of those that a mesh axis runs over, the one named last changes fastest.
Arguments:
- right_sides: bfloat16 [512, 131072], P('rhs', 'leaf'), may hold values from -6 to 6
- block_order: int32 [1024], replicated, may hold values from 0 to 1023, each once
- leaf_basis: bfloat16 [128, 1024, 256], P('leaf'), may hold values from -0.1875 to 0.1875
- leaf_inner: bfloat16 [128, 256, 256], P('leaf'), may hold values from -0.375 to 0.375
- leaf_inverse: bfloat16 [128, 768, 768], P('leaf', 'rhs'), may hold values from -0.21875 to 0.21875
- leaf_coupling: bfloat16 [128, 768, 256], P('leaf'), may hold values from -0.21875 to 0.21875
- merge_one: bfloat16 [32768, 512], P('leaf'), may hold values from -0.25 to 0.25
- merge_two: bfloat16 [16384, 512], P('leaf'), may hold values from -0.25 to 0.25
- merge_three: bfloat16 [8192, 512], P('leaf'), may hold values from -0.25 to 0.25
Outputs:
- leaf_part: bfloat16 [512, 98304], P('rhs', 'leaf')
- level_one: float32 [512, 16384], P('rhs', 'leaf')
- level_two: float32 [512, 8192], P('rhs', 'leaf')
- level_three: float32 [512, 4096], P('rhs', 'leaf')
- top_skeleton: float32 [512, 4096], P('rhs', 'leaf')
The draws below stay inside these ranges and needn't reach their ends.
Inputs may be any that keep to these rules, and one draw needn't show every extreme that they name: block_order is a permutation: every block of the 1024 appears exactly once.
All inputs are finite; a program needn't handle non-finite values.
Results may differ from the reference program's by a relative error of at most 0.007.
Values may be sent and summed in bfloat16 or wider, within the bound.
A program may use at most 64 MiB of HBM per device.

```python
import jax
import jax.numpy as jnp
from jax import lax

M = 1024
R = 256
BLOCK = 128
E = 768
LEAVES = 128
NRHS = 512
N = 131072
NBLK = 1024


def levels(rng, extent, cuts, least, largest):
    level, own = 1.0, jax.random.fold_in(rng, 6)
    for position, parts in cuts:
        heights = jnp.exp(jax.random.uniform(jax.random.fold_in(own, position), (parts,), jnp.float32, least / len(cuts), largest / len(cuts)))
        level = level * jnp.repeat(heights, extent[position] // parts).reshape([-1 if axis == position else 1 for axis in range(len(extent))])
    return level


def scatter_about(rng, extent, scale, most, split=(), dtype=jnp.bfloat16):
    result = jax.random.normal(rng, extent, jnp.float32) * scale
    if len(split) > 0:
        result = levels(rng, extent, split, -0.22, 0.18) * result
    return jnp.clip(result, min=-most, max=most).astype(dtype)


def setup_inputs(seed: int = 0) -> dict:
    seeds = jax.random.split(jax.random.key(seed), 10)
    right_sides = scatter_about(seeds[0], (NRHS, N), 1.0, 6.0, ((0, 4), (1, 128)))
    block_order = jax.random.permutation(seeds[1], NBLK).astype(jnp.int32)
    leaf_basis = scatter_about(seeds[2], (LEAVES, M, R), M ** -0.5, 0.1875, ((0, 128),))
    leaf_inner = scatter_about(seeds[3], (LEAVES, R, R), R ** -0.5, 0.375, ((0, 128),))
    leaf_inverse = scatter_about(seeds[4], (LEAVES, E, E), E ** -0.5, 0.21875, ((0, 128), (1, 4)))
    leaf_coupling = scatter_about(seeds[5], (LEAVES, E, R), E ** -0.5, 0.21875, ((0, 128),))
    merge_one = scatter_about(seeds[6], (LEAVES * R, 2 * R), (2 * R) ** -0.5, 0.25, ((0, 128),))
    merge_two = scatter_about(seeds[7], (LEAVES * R // 2, 2 * R), (2 * R) ** -0.5, 0.25, ((0, 128),))
    merge_three = scatter_about(seeds[8], (LEAVES * R // 4, 2 * R), (2 * R) ** -0.5, 0.25, ((0, 128),))
    return dict(right_sides=right_sides, block_order=block_order, leaf_basis=leaf_basis, leaf_inner=leaf_inner, leaf_inverse=leaf_inverse, leaf_coupling=leaf_coupling, merge_one=merge_one, merge_two=merge_two, merge_three=merge_three)


def reference(right_sides, block_order, leaf_basis, leaf_inner, leaf_inverse, leaf_coupling, merge_one, merge_two, merge_three):
    blocks = right_sides.reshape(NRHS, NBLK, BLOCK)
    tree_order = jnp.take(blocks, block_order.astype(jnp.int32), axis=1).reshape(NRHS, LEAVES, M)
    tree_order = jnp.transpose(tree_order, (1, 0, 2))

    def one_leaf(leaf_items):
        local_rows, basis_matrix, inner_matrix, inverse, coupling = leaf_items
        projected = jnp.dot(local_rows, basis_matrix, preferred_element_type=jnp.float32).astype(jnp.bfloat16)
        middle = jnp.dot(projected, inner_matrix, preferred_element_type=jnp.float32).astype(jnp.bfloat16)
        correction = jnp.dot(middle, basis_matrix.T, preferred_element_type=jnp.float32)
        reflected = (local_rows.astype(jnp.float32) - correction).astype(jnp.bfloat16)
        eliminated = jnp.dot(reflected[:, :E], inverse, preferred_element_type=jnp.float32).astype(jnp.bfloat16)
        skeleton = (reflected[:, E:].astype(jnp.float32) - jnp.dot(eliminated, coupling, preferred_element_type=jnp.float32)).astype(jnp.bfloat16)
        return eliminated, skeleton

    eliminated, skeleton = lax.map(one_leaf, (tree_order, leaf_basis, leaf_inner, leaf_inverse, leaf_coupling))
    leaf_part = jnp.transpose(eliminated, (1, 0, 2)).reshape(NRHS, LEAVES * E)
    current = jnp.transpose(skeleton, (1, 0, 2))
    outputs = []
    node_count = LEAVES
    upper_part = None
    for level_index, merge_table in enumerate((merge_one, merge_two, merge_three), start=1):
        node_count = node_count // 2
        group_count = 2 ** level_index
        paired = current.reshape(NRHS, node_count, 2 * R).astype(jnp.float32)
        operators = merge_table.reshape(node_count, 2 * R, 2 * R).astype(jnp.float32)
        joined = jnp.einsum("cpk,pkj->cpj", paired, operators)
        joined = joined.reshape(NRHS, node_count, group_count, 2, R // group_count)
        outputs.append(joined[:, :, :, 0, :].reshape(NRHS, node_count * R))
        upper_part = joined[:, :, :, 1, :].reshape(NRHS, node_count, R)
        current = upper_part.astype(jnp.bfloat16)
    return (leaf_part, outputs[0], outputs[1], outputs[2], upper_part.reshape(NRHS, node_count * R))
```

```python
import jax
import jax.numpy as jnp
from jax import lax
from jax.experimental import pallas as pl
from jax.experimental.pallas import tpu as pltpu
from jax.sharding import PartitionSpec as P

BF = jnp.bfloat16
F32 = jnp.float32
CHIPS = 64
GROUP = 8
PLANES = 4


def dot(a, b):
    return jnp.dot(a, b, preferred_element_type=F32)


def kernel(
    order,
    rows_in,
    basis_in,
    inner_in,
    inverse_in,
    coupling_in,
    one_in,
    two_in,
    three_in,
    leaf_out,
    first_out,
    second_out,
    third_out,
    top_out,
    rows,
    pool,
    picked,
    placed,
    flat,
    basis,
    inner,
    inverse,
    coupling,
    one,
    two,
    three,
    w_one,
    w_two,
    w_three,
    s_one,
    s_two,
    s_three,
    o_leaf,
    o_first,
    o_second,
    o_third,
    o_top,
    load_sem,
    own_sem,
    out_sem,
    spread_sem,
    twin_sem,
    gather_sem,
    inv_sem,
    w_sem,
    s_sem,
):
    me = lax.axis_index("leaf")
    plane = lax.axis_index("rhs")
    chip = me // 2
    core = me % 2
    in_group = me % GROUP
    group = me - in_group
    in_quad = me % 4
    quad = me - in_quad
    twin = me + 1 - 2 * core

    loads = [
        (rows_in, rows),
        (inverse_in, inverse.at[pl.ds(pl.multiple_of(plane * 192, 64), 192)]),
        (one_in, one),
        (two_in, two),
        (three_in, three),
        (basis_in, basis),
        (inner_in, inner),
        (coupling_in, coupling),
    ]
    loads = [pltpu.make_async_copy(a, b, load_sem.at[i]) for i, (a, b) in enumerate(loads)]
    for load in loads:
        load.start()

    def remote(src, dst, send, recv, target, axis="leaf"):
        return pltpu.make_async_remote_copy(
            src_ref=src,
            dst_ref=dst,
            send_sem=send,
            recv_sem=recv,
            device_id={axis: target},
            device_id_type=pl.DeviceIdType.MESH,
        )

    barrier = pltpu.get_barrier_semaphore()

    def greet(target, axis="leaf"):
        pl.semaphore_signal(
            barrier, inc=1, device_id={axis: target}, device_id_type=pl.DeviceIdType.MESH
        )

    def greet_chip(k, _):
        greet(lax.rem(chip + k, CHIPS) * 2 + core)
        return 0

    lax.fori_loop(1, CHIPS, greet_chip, 0)
    for i in range(GROUP // 2):
        greet(group + 2 * i + 1 - core)
    for d in range(1, PLANES):
        greet(lax.rem(plane + d, PLANES), "rhs")
    pl.semaphore_wait(barrier, CHIPS - 1 + GROUP // 2 + PLANES - 1)

    loads[0].wait()
    mine = pl.ds(pl.multiple_of((core * CHIPS + chip) * 8, 8), 8)

    def spread(k, _):
        other = lax.rem(chip + k, CHIPS)
        remote(
            rows.at[other // 4, :, other % 4],
            pool.at[mine],
            spread_sem.at[0],
            spread_sem.at[1],
            other * 2 + core,
        ).start()
        return 0

    lax.fori_loop(1, CHIPS, spread, 0)
    own = pltpu.make_async_copy(rows.at[chip // 4, :, chip % 4], pool.at[mine], own_sem.at[0])
    own.start()

    pieces = []
    for load in loads[1:5]:
        load.wait()
    for d in range(1, PLANES):
        share = inverse.at[pl.ds(pl.multiple_of(plane * 192, 64), 192)]
        c = remote(
            share, share, inv_sem.at[0, d], inv_sem.at[1, d], lax.rem(plane + d, PLANES), "rhs"
        )
        c.start()
        pieces.append(c)
    c = remote(
        one.at[:, pl.ds(pl.multiple_of((1 - core) * 256, 256), 256)],
        w_one.at[core],
        w_sem.at[0, 0],
        w_sem.at[1, 0],
        twin,
    )
    c.start()
    pieces.append(c)
    local = [
        pltpu.make_async_copy(
            one.at[:, pl.ds(pl.multiple_of(core * 256, 256), 256)], w_one.at[core], own_sem.at[1]
        ),
        pltpu.make_async_copy(
            two.at[:, pl.ds(pl.multiple_of(in_quad * 128, 128), 128)],
            w_two.at[in_quad],
            own_sem.at[2],
        ),
        pltpu.make_async_copy(
            three.at[:, pl.ds(pl.multiple_of(in_group // 2 * 128, 128), 128)],
            w_three.at[in_group],
            own_sem.at[3],
        ),
    ]
    for c in local:
        c.start()
    for d in range(1, 4):
        other = lax.rem(in_quad + d, 4)
        c = remote(
            two.at[:, pl.ds(pl.multiple_of(other * 128, 128), 128)],
            w_two.at[in_quad],
            w_sem.at[0, d],
            w_sem.at[1, d],
            quad + other,
        )
        c.start()
        pieces.append(c)
    for d in range(1, GROUP):
        other = lax.rem(in_group + d, GROUP)
        c = remote(
            three.at[:, pl.ds(pl.multiple_of(other // 2 * 128, 128), 128)],
            w_three.at[in_group],
            w_sem.at[0, 3 + d],
            w_sem.at[1, 3 + d],
            group + other,
        )
        c.start()
        pieces.append(c)

    own.wait()
    part = pool.at[pl.ds(0, (CHIPS - 1) * 8)]
    pltpu.make_async_copy(part, part, spread_sem.at[1]).wait()
    half = pool.at[pl.ds(pl.multiple_of(core * CHIPS * 8, 8), CHIPS * 8)]
    handed = remote(half, half, twin_sem.at[0], twin_sem.at[1], twin)
    handed.start()
    handed.wait_recv()

    def send(other):
        remote(
            picked.at[other],
            placed.at[:, chip],
            gather_sem.at[0],
            gather_sem.at[1],
            other * 2 + core,
        ).start()

    def gather(k, _):
        other = lax.rem(chip + k, CHIPS)
        first = (other * 2 + core) * 8
        for j in range(8):
            picked[other, j] = pool[order[first + j]]

        @pl.when(k > 1)
        def _():
            send(lax.rem(chip + k - 1, CHIPS))

        return 0

    lax.fori_loop(1, CHIPS + 1, gather, 0)
    own = pltpu.make_async_copy(picked.at[chip], placed.at[:, chip], own_sem.at[0])
    own.start()
    for load in loads[5:]:
        load.wait()
    own.wait()
    part = picked.at[pl.ds(0, CHIPS - 1)]
    pltpu.make_async_copy(part, part, gather_sem.at[1]).wait()

    for j in range(8):
        flat[:, j * 128 : (j + 1) * 128] = placed[j].reshape(128, 128)
    projected = dot(flat[...], basis[...]).astype(BF)
    middle = dot(projected, inner[...]).astype(BF)
    correction = lax.dot_general(
        middle, basis[...], (((1,), (1,)), ((), ())), preferred_element_type=F32
    )
    reflected = (flat[...].astype(F32) - correction).astype(BF)
    for c in pieces[:3]:
        c.wait_recv()
    eliminated = dot(reflected[:, :768], inverse[...]).astype(BF)
    o_leaf[...] = eliminated
    outs = [pltpu.make_async_copy(o_leaf, leaf_out, out_sem.at[0])]
    outs[0].start()
    coupled = dot(eliminated, coupling[...])
    s_one[core] = (reflected[:, 768:].astype(F32) - coupled).astype(BF)

    c = remote(s_one.at[core], s_one.at[core], s_sem.at[0, 0], s_sem.at[1, 0], twin)
    c.start()
    pieces[3].wait_recv()
    local[0].wait()
    c.wait_recv()
    pieces.append(c)
    joined = dot(s_one[0], w_one[0]) + dot(s_one[1], w_one[1])
    s_two[in_quad] = joined[:, 128:].astype(BF)

    arriving = []
    for d in range(1, 4):
        c = remote(
            s_two.at[in_quad],
            s_two.at[in_quad],
            s_sem.at[0, d],
            s_sem.at[1, d],
            quad + lax.rem(in_quad + d, 4),
        )
        c.start()
        arriving.append(c)
    o_first[...] = joined[:, :128]
    outs.append(pltpu.make_async_copy(o_first, first_out, out_sem.at[1]))
    outs[-1].start()
    for c in pieces[4:7]:
        c.wait_recv()
    local[1].wait()
    for c in arriving:
        c.wait_recv()
    pieces += arriving
    joined = dot(s_two[0], w_two[0])
    for i in range(1, 4):
        joined += dot(s_two[i], w_two[i])
    s_three[in_group] = joined[:, 64:].astype(BF)

    arriving = []
    for d in range(1, GROUP):
        c = remote(
            s_three.at[in_group],
            s_three.at[in_group],
            s_sem.at[0, 3 + d],
            s_sem.at[1, 3 + d],
            group + lax.rem(in_group + d, GROUP),
        )
        c.start()
        arriving.append(c)
    o_second[...] = joined[:, :64]
    outs.append(pltpu.make_async_copy(o_second, second_out, out_sem.at[2]))
    outs[-1].start()
    for c in pieces[7:14]:
        c.wait_recv()
    local[2].wait()
    for c in arriving:
        c.wait_recv()
    pieces += arriving
    joined = dot(s_three[0], w_three[0])
    for i in range(1, GROUP):
        joined += dot(s_three[i], w_three[i])
    joined = jnp.where(in_group % 2 == 1, joined[:, 64:], joined[:, :64])
    o_third[...] = joined[:, :32]
    o_top[...] = joined[:, 32:]
    outs.append(pltpu.make_async_copy(o_third, third_out, out_sem.at[3]))
    outs.append(pltpu.make_async_copy(o_top, top_out, out_sem.at[4]))
    for c in outs[3:]:
        c.start()

    handed.wait_send()
    part = pool.at[pl.ds(0, (CHIPS - 1) * 8)]
    pltpu.make_async_copy(part, part, spread_sem.at[0]).wait()
    part = picked.at[pl.ds(0, CHIPS - 1)]
    pltpu.make_async_copy(part, part, gather_sem.at[0]).wait()
    for c in pieces:
        c.wait_send()
    for c in outs:
        c.wait()


def shards(right_sides, block_order, basis, inner, inverse, coupling, one, two, three):
    rows = right_sides.reshape(16, 4, 2, 8, 128).transpose(0, 3, 1, 2, 4)
    leaf = block_order // 8
    order = leaf % 2 * (CHIPS * 8) + leaf // 2 * 8 + block_order % 8
    anywhere = pl.BlockSpec(memory_space=pl.ANY)
    return pl.pallas_call(
        kernel,
        out_shape=(
            jax.ShapeDtypeStruct((128, 768), BF),
            jax.ShapeDtypeStruct((128, 128), F32),
            jax.ShapeDtypeStruct((128, 64), F32),
            jax.ShapeDtypeStruct((128, 32), F32),
            jax.ShapeDtypeStruct((128, 32), F32),
        ),
        in_specs=[pl.BlockSpec(memory_space=pltpu.SMEM)] + [anywhere] * 8,
        out_specs=(anywhere,) * 5,
        scratch_shapes=[
            pltpu.VMEM((16, 8, 4, 2, 128), BF),
            pltpu.VMEM((1024, 2, 128), BF),
            pltpu.VMEM((CHIPS, 8, 2, 128), BF),
            pltpu.VMEM((8, CHIPS, 2, 128), BF),
            pltpu.VMEM((128, 1024), BF),
            pltpu.VMEM((1024, 256), BF),
            pltpu.VMEM((256, 256), BF),
            pltpu.VMEM((768, 768), BF),
            pltpu.VMEM((768, 256), BF),
            pltpu.VMEM((256, 512), BF),
            pltpu.VMEM((128, 512), BF),
            pltpu.VMEM((64, 512), BF),
            pltpu.VMEM((2, 256, 256), BF),
            pltpu.VMEM((4, 128, 128), BF),
            pltpu.VMEM((GROUP, 64, 128), BF),
            pltpu.VMEM((2, 128, 256), BF),
            pltpu.VMEM((4, 128, 128), BF),
            pltpu.VMEM((GROUP, 128, 64), BF),
            pltpu.VMEM((128, 768), BF),
            pltpu.VMEM((128, 128), F32),
            pltpu.VMEM((128, 64), F32),
            pltpu.VMEM((128, 32), F32),
            pltpu.VMEM((128, 32), F32),
            pltpu.SemaphoreType.DMA((8,)),
            pltpu.SemaphoreType.DMA((4,)),
            pltpu.SemaphoreType.DMA((5,)),
            pltpu.SemaphoreType.DMA((2,)),
            pltpu.SemaphoreType.DMA((2,)),
            pltpu.SemaphoreType.DMA((2,)),
            pltpu.SemaphoreType.DMA((2, 4)),
            pltpu.SemaphoreType.DMA((2, 11)),
            pltpu.SemaphoreType.DMA((2, 11)),
        ],
        compiler_params=pltpu.CompilerParams(collective_id=0, has_side_effects=True),
    )(order, rows, basis[0], inner[0], inverse[0], coupling[0], one, two, three)


def solution(mesh):
    return jax.shard_map(
        shards,
        mesh=mesh,
        in_specs=(
            P("rhs", "leaf"),
            P(),
            P("leaf", None, None),
            P("leaf", None, None),
            P("leaf", "rhs", None),
            P("leaf", None, None),
            P("leaf", None),
            P("leaf", None),
            P("leaf", None),
        ),
        out_specs=(P("rhs", "leaf"),) * 5,
        check_vma=False,
    )
```

```python
import jax
import jax.numpy as jnp
from jax import lax
from jax.experimental import pallas as pl
from jax.experimental.pallas import tpu as pltpu
from jax.sharding import PartitionSpec as P

BF = jnp.bfloat16
F32 = jnp.float32
CHIPS = 64
GROUP = 8
PLANES = 4


def dot(a, b):
    return jnp.dot(a, b, preferred_element_type=F32)


def kernel(
    order_in,
    rows_in,
    basis_in,
    inner_in,
    inverse_in,
    coupling_in,
    one_in,
    two_in,
    three_in,
    leaf_out,
    first_out,
    second_out,
    last_out,
    order,
    rows,
    pool,
    picked,
    placed,
    flat,
    basis,
    inner,
    inverse,
    coupling,
    one,
    two,
    three,
    w_one,
    w_two,
    w_three,
    w_wide,
    s_one,
    s_two,
    s_three,
    load_sem,
    own_sem,
    spread_sem,
    twin_sem,
    gather_sem,
    inv_sem,
    w_sem,
    s_sem,
):
    me = lax.axis_index("leaf")
    plane = lax.axis_index("rhs")
    chip = me // 2
    core = me % 2
    in_group = me % GROUP
    group = me - in_group
    in_quad = me % 4
    quad = me - in_quad
    twin = me + 1 - 2 * core
    row, column = chip // 8, chip % 8

    loads = [
        (rows_in, rows),
        (inverse_in, inverse.at[pl.ds(pl.multiple_of(plane * 192, 64), 192)]),
        (one_in, one),
        (two_in, two),
        (three_in, three),
        (basis_in, basis),
        (inner_in, inner),
        (coupling_in, coupling),
        (order_in, order),
    ]
    loads = [pltpu.make_async_copy(a, b, load_sem.at[i]) for i, (a, b) in enumerate(loads)]
    for load in loads:
        load.start()

    def remote(src, dst, send, recv, target, axis="leaf"):
        return pltpu.make_async_remote_copy(
            src_ref=src,
            dst_ref=dst,
            send_sem=send,
            recv_sem=recv,
            device_id={axis: target},
            device_id_type=pl.DeviceIdType.MESH,
        )

    barrier = pltpu.get_barrier_semaphore()

    def greet(target, axis="leaf"):
        pl.semaphore_signal(
            barrier, inc=1, device_id={axis: target}, device_id_type=pl.DeviceIdType.MESH
        )

    def greet_chip(k, _):
        greet(lax.rem(chip + k, CHIPS) * 2 + core)
        return 0

    lax.fori_loop(1, CHIPS, greet_chip, 0)
    for i in range(GROUP // 2):
        greet(group + 2 * i + 1 - core)
    for d in range(1, PLANES):
        greet(lax.rem(plane + d, PLANES), "rhs")
    pl.semaphore_wait(barrier, CHIPS - 1 + GROUP // 2 + PLANES - 1)

    loads[0].wait()
    mine = pl.ds(pl.multiple_of(me * 8, 8), 8)

    def step(i):
        far = (8 - i) // 2
        return far + (1 - i % 2) * (1 - i // 7) * lax.rem(8 - 2 * far, 8)

    def target(i):
        return lax.rem(row + step(i // 8), 8) * 8 + lax.rem(column + step(i % 8), 8)

    def spread(i, _):
        other = target(i)
        remote(
            rows.at[other // 4, :, other % 4],
            pool.at[mine],
            spread_sem.at[8],
            spread_sem.at[i // 8],
            other * 2 + core,
        ).start()
        return 0

    lax.fori_loop(0, CHIPS - 1, spread, 0)
    own = pltpu.make_async_copy(rows.at[chip // 4, :, chip % 4], pool.at[mine], own_sem.at[0])
    own.start()

    pieces = []
    loads[1].wait()
    for d in range(1, PLANES):
        share = inverse.at[pl.ds(pl.multiple_of(plane * 192, 64), 192)]
        c = remote(
            share, share, inv_sem.at[0, d], inv_sem.at[1, d], lax.rem(plane + d, PLANES), "rhs"
        )
        c.start()
        pieces.append(c)
    def hand(i, count):
        part = pool.at[pl.ds(0, count * 8)]
        pltpu.make_async_copy(part, part, spread_sem.at[i]).wait()
        origin = lax.rem(row + 8 - step(i), 8)

        def one_leaf(y, _):
            block = pool.at[pl.ds(pl.multiple_of(((origin * 8 + y) * 2 + core) * 8, 8), 8)]
            remote(block, block, twin_sem.at[0], twin_sem.at[1], twin).start()
            return 0

        lax.fori_loop(0, 8, one_leaf, 0)
        return 0

    lax.fori_loop(0, 7, lambda i, _: hand(i, 8), 0)
    own.wait()
    hand(7, 7)
    loads[8].wait()
    half = pool.at[pl.ds(0, CHIPS * 8)]
    pltpu.make_async_copy(half, half, twin_sem.at[1]).wait()

    def send(other):
        remote(
            picked.at[other],
            placed.at[:, chip],
            gather_sem.at[0],
            gather_sem.at[1],
            other * 2 + core,
        ).start()

    def gather(i, _):
        other = target(i)
        first = (other * 2 + core) * 8
        for j in range(8):
            picked[other, j] = pool[order[first + j]]

        @pl.when(i > 0)
        def _():
            send(target(i - 1))

        return 0

    lax.fori_loop(0, CHIPS, gather, 0)
    own = pltpu.make_async_copy(picked.at[chip], placed.at[:, chip], own_sem.at[0])
    own.start()
    for load in loads[2:5]:
        load.wait()
    c = remote(
        one.at[:, pl.ds(pl.multiple_of((1 - core) * 256, 256), 256)],
        w_one.at[core],
        w_sem.at[0, 0],
        w_sem.at[1, 0],
        twin,
    )
    c.start()
    pieces.append(c)
    local = [
        pltpu.make_async_copy(
            one.at[:, pl.ds(pl.multiple_of(core * 256, 256), 256)], w_one.at[core], own_sem.at[1]
        ),
        pltpu.make_async_copy(
            two.at[:, pl.ds(pl.multiple_of(in_quad * 128, 128), 128)],
            w_two.at[in_quad],
            own_sem.at[2],
        ),
        pltpu.make_async_copy(
            three.at[:, pl.ds(pl.multiple_of(in_group // 2 * 128, 128), 128)],
            w_three.at[in_group],
            own_sem.at[3],
        ),
    ]
    for c in local:
        c.start()
    for d in range(1, 4):
        other = lax.rem(in_quad + d, 4)
        c = remote(
            two.at[:, pl.ds(pl.multiple_of(other * 128, 128), 128)],
            w_two.at[in_quad],
            w_sem.at[0, d],
            w_sem.at[1, d],
            quad + other,
        )
        c.start()
        pieces.append(c)
    for d in range(1, GROUP):
        other = lax.rem(in_group + d, GROUP)
        c = remote(
            three.at[:, pl.ds(pl.multiple_of(other // 2 * 128, 128), 128)],
            w_three.at[in_group],
            w_sem.at[0, 3 + d],
            w_sem.at[1, 3 + d],
            group + other,
        )
        c.start()
        pieces.append(c)
    for load in loads[5:8]:
        load.wait()
    own.wait()
    part = picked.at[pl.ds(0, CHIPS - 1)]
    pltpu.make_async_copy(part, part, gather_sem.at[1]).wait()

    for j in range(8):
        flat[:, j * 128 : (j + 1) * 128] = placed[j].reshape(128, 128)
    projected = dot(flat[...], basis[...]).astype(BF)
    middle = dot(projected, inner[...]).astype(BF)
    correction = lax.dot_general(
        middle, basis[...], (((1,), (1,)), ((), ())), preferred_element_type=F32
    )
    reflected = (flat[...].astype(F32) - correction).astype(BF)
    for c in pieces[:3]:
        c.wait_recv()
    eliminated = dot(reflected[:, :768], inverse[...]).astype(BF)
    leaf_out[...] = eliminated
    coupled = dot(eliminated, coupling[...])
    s_one[core] = (reflected[:, 768:].astype(F32) - coupled).astype(BF)

    c = remote(s_one.at[core], s_one.at[core], s_sem.at[0, 0], s_sem.at[1, 0], twin)
    c.start()
    pieces[3].wait_recv()
    local[0].wait()
    c.wait_recv()
    pieces.append(c)
    joined = dot(s_one[0], w_one[0]) + dot(s_one[1], w_one[1])
    s_two[in_quad] = joined[:, 128:].astype(BF)

    arriving = []
    for d in range(1, 4):
        c = remote(
            s_two.at[in_quad],
            s_two.at[in_quad],
            s_sem.at[0, d],
            s_sem.at[1, d],
            quad + lax.rem(in_quad + d, 4),
        )
        c.start()
        arriving.append(c)
    first_out[...] = joined[:, :128]
    for c in pieces[4:7]:
        c.wait_recv()
    local[1].wait()
    for c in arriving:
        c.wait_recv()
    pieces += arriving
    joined = dot(s_two[0], w_two[0])
    for i in range(1, 4):
        joined += dot(s_two[i], w_two[i])
    low = lax.broadcasted_iota(jnp.int32, (64, 128), 1) < 64
    s_three[in_group] = jnp.where(low, pltpu.roll(joined[:64], 64, 1), joined[64:]).astype(BF)

    arriving = []
    for d in range(1, GROUP):
        c = remote(
            s_three.at[in_group],
            s_three.at[in_group],
            s_sem.at[0, 3 + d],
            s_sem.at[1, 3 + d],
            group + lax.rem(in_group + d, GROUP),
        )
        c.start()
        arriving.append(c)
    second_out[...] = joined.T[:64]
    for c in pieces[7:14]:
        c.wait_recv()
    local[2].wait()
    odd = in_group % 2 == 1
    for i in range(GROUP):
        w = w_three[i].astype(F32)
        turned = pltpu.roll(w, 64, 1)
        w_wide[i, :64] = jnp.where(low, jnp.where(odd, turned, w), 0.0).astype(BF)
        w_wide[i, 64:] = jnp.where(low, 0.0, jnp.where(odd, w, turned)).astype(BF)
    for c in arriving:
        c.wait_recv()
    pieces += arriving
    joined = dot(s_three[0], w_wide[0])
    for i in range(1, GROUP):
        joined += dot(s_three[i], w_wide[i])
    turned = joined.T
    last_out[:, :64] = turned[:64]
    last_out[:, 64:] = turned[64:]

    pltpu.make_async_copy(half, half, twin_sem.at[0]).wait()
    part = pool.at[pl.ds(0, (CHIPS - 1) * 8)]
    pltpu.make_async_copy(part, part, spread_sem.at[8]).wait()
    part = picked.at[pl.ds(0, CHIPS - 1)]
    pltpu.make_async_copy(part, part, gather_sem.at[0]).wait()
    for c in pieces:
        c.wait_send()


def finish(leaf_in, first_in, second_in, last_in, leaf, first, second, third, top):
    leaf[...] = leaf_in[...]
    first[...] = first_in[...]
    second[...] = second_in[...]
    third[...] = last_in[:32]
    top[...] = last_in[32:]


def shards(right_sides, block_order, basis, inner, inverse, coupling, one, two, three):
    rows = right_sides.reshape(16, 4, 2, 8, 128).transpose(0, 3, 1, 2, 4)
    anywhere = pl.BlockSpec(memory_space=pl.ANY)
    vmem = pl.BlockSpec(memory_space=pltpu.VMEM)
    results = pl.pallas_call(
        kernel,
        out_shape=(
            jax.ShapeDtypeStruct((128, 768), BF),
            jax.ShapeDtypeStruct((128, 128), F32),
            jax.ShapeDtypeStruct((64, 128), F32),
            jax.ShapeDtypeStruct((64, 128), F32),
        ),
        in_specs=[anywhere] * 9,
        out_specs=(vmem,) * 4,
        scratch_shapes=[
            pltpu.SMEM((1024,), jnp.int32),
            pltpu.VMEM((16, 8, 4, 2, 128), BF),
            pltpu.VMEM((1024, 2, 128), BF),
            pltpu.VMEM((CHIPS, 8, 2, 128), BF),
            pltpu.VMEM((8, CHIPS, 2, 128), BF),
            pltpu.VMEM((128, 1024), BF),
            pltpu.VMEM((1024, 256), BF),
            pltpu.VMEM((256, 256), BF),
            pltpu.VMEM((768, 768), BF),
            pltpu.VMEM((768, 256), BF),
            pltpu.VMEM((256, 512), BF),
            pltpu.VMEM((128, 512), BF),
            pltpu.VMEM((64, 512), BF),
            pltpu.VMEM((2, 256, 256), BF),
            pltpu.VMEM((4, 128, 128), BF),
            pltpu.VMEM((GROUP, 64, 128), BF),
            pltpu.VMEM((GROUP, 128, 128), BF),
            pltpu.VMEM((2, 128, 256), BF),
            pltpu.VMEM((4, 128, 128), BF),
            pltpu.VMEM((GROUP, 64, 128), BF),
            pltpu.SemaphoreType.DMA((9,)),
            pltpu.SemaphoreType.DMA((4,)),
            pltpu.SemaphoreType.DMA((9,)),
            pltpu.SemaphoreType.DMA((2,)),
            pltpu.SemaphoreType.DMA((2,)),
            pltpu.SemaphoreType.DMA((2, 4)),
            pltpu.SemaphoreType.DMA((2, 11)),
            pltpu.SemaphoreType.DMA((2, 11)),
        ],
        compiler_params=pltpu.CompilerParams(collective_id=0, has_side_effects=True),
    )(block_order, rows, basis[0], inner[0], inverse[0], coupling[0], one, two, three)
    leaf, first, second, third, top = pl.pallas_call(
        finish,
        out_shape=(
            jax.ShapeDtypeStruct((128, 768), BF),
            jax.ShapeDtypeStruct((128, 128), F32),
            jax.ShapeDtypeStruct((64, 128), F32),
            jax.ShapeDtypeStruct((32, 128), F32),
            jax.ShapeDtypeStruct((32, 128), F32),
        ),
        in_specs=[vmem] * 4,
        out_specs=(vmem,) * 5,
    )(*results)
    return leaf, first, second.T, third.T, top.T


def solution(mesh):
    return jax.shard_map(
        shards,
        mesh=mesh,
        in_specs=(
            P("rhs", "leaf"),
            P(),
            P("leaf", None, None),
            P("leaf", None, None),
            P("leaf", "rhs", None),
            P("leaf", None, None),
            P("leaf", None),
            P("leaf", None),
            P("leaf", None),
        ),
        out_specs=(P("rhs", "leaf"),) * 5,
        check_vma=False,
    )
```

```python
import jax
import jax.numpy as jnp
from jax import lax
from jax.experimental import pallas as pl
from jax.experimental.pallas import tpu as pltpu
from jax.sharding import PartitionSpec as P

BF = jnp.bfloat16
F32 = jnp.float32
CHIPS = 64
GROUP = 8
PLANES = 4
STEPS = (4, 3, 5, 2, 6, 1, 7, 0)


def dot(a, b):
    return jnp.dot(a, b, preferred_element_type=F32)


def kernel(
    order_in,
    rows_in,
    basis_in,
    inner_in,
    inverse_in,
    coupling_in,
    one_in,
    two_in,
    three_in,
    leaf_out,
    first_out,
    second_out,
    last_out,
    order,
    rows,
    pool,
    picked,
    placed,
    flat,
    basis,
    inner,
    inverse,
    coupling,
    whole,
    leading,
    one,
    two,
    three,
    w_one,
    w_two,
    w_three,
    w_wide,
    s_one,
    s_two,
    s_three,
    load_sem,
    own_sem,
    spread_sem,
    twin_sem,
    gather_sem,
    inv_sem,
    w_sem,
    s_sem,
):
    me = lax.axis_index("leaf")
    plane = lax.axis_index("rhs")
    chip = me // 2
    core = me % 2
    in_group = me % GROUP
    group = me - in_group
    in_quad = me % 4
    quad = me - in_quad
    twin = me + 1 - 2 * core
    row, column = chip // 8, chip % 8

    loads = [
        (rows_in, rows),
        (inverse_in, inverse.at[pl.ds(pl.multiple_of(plane * 192, 64), 192)]),
        (one_in, one),
        (two_in, two),
        (three_in, three),
        (basis_in, basis),
        (inner_in, inner),
        (coupling_in, coupling),
        (order_in, order),
    ]
    loads = [pltpu.make_async_copy(a, b, load_sem.at[i]) for i, (a, b) in enumerate(loads)]
    for load in loads:
        load.start()

    def remote(src, dst, send, recv, target, axis="leaf"):
        return pltpu.make_async_remote_copy(
            src_ref=src,
            dst_ref=dst,
            send_sem=send,
            recv_sem=recv,
            device_id={axis: target},
            device_id_type=pl.DeviceIdType.MESH,
        )

    def step(i):
        far = (8 - i) // 2
        return far + (1 - i % 2) * (1 - i // 7) * lax.rem(8 - 2 * far, 8)

    columns = [lax.rem(column + STEPS[j], 8) for j in range(8)]

    def each_chip(visit):
        def one_row(i, _):
            first = lax.rem(row + step(i), 8) * 8
            for j in range(8):
                visit(first + columns[j], i)
            return 0

        lax.fori_loop(0, 7, one_row, 0)
        for j in range(7):
            visit(row * 8 + columns[j], 7)

    barrier = pltpu.get_barrier_semaphore()

    def greet(target, axis="leaf"):
        pl.semaphore_signal(
            barrier, inc=1, device_id={axis: target}, device_id_type=pl.DeviceIdType.MESH
        )

    each_chip(lambda other, i: greet(other * 2 + core))
    for i in range(GROUP // 2):
        greet(group + 2 * i + 1 - core)
    for d in range(1, PLANES):
        greet(lax.rem(plane + d, PLANES), "rhs")
    pl.semaphore_wait(barrier, CHIPS - 1 + GROUP // 2 + PLANES - 1)

    loads[0].wait()
    mine = pl.ds(pl.multiple_of(me * 8, 8), 8)

    def spread(other, i):
        remote(
            rows.at[other // 4, :, other % 4],
            pool.at[mine],
            spread_sem.at[8],
            spread_sem.at[i],
            other * 2 + core,
        ).start()

    each_chip(spread)
    own = pltpu.make_async_copy(rows.at[chip // 4, :, chip % 4], pool.at[mine], own_sem.at[0])
    own.start()

    pieces = []
    loads[1].wait()
    for d in range(1, PLANES):
        share = inverse.at[pl.ds(pl.multiple_of(plane * 192, 64), 192)]
        c = remote(
            share, share, inv_sem.at[0, d], inv_sem.at[1, d], lax.rem(plane + d, PLANES), "rhs"
        )
        c.start()
        pieces.append(c)
    def hand(i, count):
        part = pool.at[pl.ds(0, count * 8)]
        pltpu.make_async_copy(part, part, spread_sem.at[i]).wait()
        origin = lax.rem(row + 8 - step(i), 8)

        def one_leaf(y, _):
            block = pool.at[pl.ds(pl.multiple_of(((origin * 8 + y) * 2 + core) * 8, 8), 8)]
            remote(block, block, twin_sem.at[0], twin_sem.at[1], twin).start()
            return 0

        lax.fori_loop(0, 8, one_leaf, 0)
        return 0

    lax.fori_loop(0, 7, lambda i, _: hand(i, 8), 0)
    own.wait()
    hand(7, 7)
    loads[8].wait()
    half = pool.at[pl.ds(0, CHIPS * 8)]
    pltpu.make_async_copy(half, half, twin_sem.at[1]).wait()

    def send(other):
        remote(
            picked.at[other],
            placed.at[:, chip],
            gather_sem.at[0],
            gather_sem.at[1],
            other * 2 + core,
        ).start()

    def pick(other):
        first = (other * 2 + core) * 8
        blocks = [pool[order[first + j]] for j in range(8)]
        for j in range(8):
            picked[other, j] = blocks[j]

    def gather(i, _):
        first = lax.rem(row + step(i), 8) * 8
        for j in range(8):
            pick(first + columns[j])
            if j > 0:
                send(first + columns[j - 1])
        send(first + columns[7])
        return 0

    lax.fori_loop(0, 7, gather, 0)
    for j in range(8):
        pick(row * 8 + columns[j])
        if j > 0:
            send(row * 8 + columns[j - 1])
    own = pltpu.make_async_copy(picked.at[chip], placed.at[:, chip], own_sem.at[0])
    own.start()
    for load in loads[2:5]:
        load.wait()
    c = remote(
        one.at[:, pl.ds(pl.multiple_of((1 - core) * 256, 256), 256)],
        w_one.at[core],
        w_sem.at[0, 0],
        w_sem.at[1, 0],
        twin,
    )
    c.start()
    pieces.append(c)
    local = [
        pltpu.make_async_copy(
            one.at[:, pl.ds(pl.multiple_of(core * 256, 256), 256)], w_one.at[core], own_sem.at[1]
        ),
        pltpu.make_async_copy(
            two.at[:, pl.ds(pl.multiple_of(in_quad * 128, 128), 128)],
            w_two.at[in_quad],
            own_sem.at[2],
        ),
        pltpu.make_async_copy(
            three.at[:, pl.ds(pl.multiple_of(in_group // 2 * 128, 128), 128)],
            w_three.at[in_group],
            own_sem.at[3],
        ),
    ]
    for c in local:
        c.start()
    for d in range(1, 4):
        other = lax.rem(in_quad + d, 4)
        c = remote(
            two.at[:, pl.ds(pl.multiple_of(other * 128, 128), 128)],
            w_two.at[in_quad],
            w_sem.at[0, d],
            w_sem.at[1, d],
            quad + other,
        )
        c.start()
        pieces.append(c)
    for d in range(1, GROUP):
        other = lax.rem(in_group + d, GROUP)
        c = remote(
            three.at[:, pl.ds(pl.multiple_of(other // 2 * 128, 128), 128)],
            w_three.at[in_group],
            w_sem.at[0, 3 + d],
            w_sem.at[1, 3 + d],
            group + other,
        )
        c.start()
        pieces.append(c)
    for load in loads[5:8]:
        load.wait()
    own.wait()

    spread_back = lax.dot_general(
        inner[...], basis[...], (((1,), (1,)), ((), ())), preferred_element_type=F32
    )
    for c in pieces[:3]:
        c.wait_recv()
    folded = dot(inverse[...], coupling[...])
    folded_low = folded.astype(BF)
    rest = spread_back[:, 768:] - dot(spread_back[:, :768].astype(BF), folded_low)
    rest = rest.astype(BF)
    whole[:768] = (folded + dot(basis[:768], rest)).astype(BF)
    whole[768:] = dot(basis[768:], rest).astype(BF)

    part = picked.at[pl.ds(0, CHIPS - 1)]
    pltpu.make_async_copy(part, part, gather_sem.at[1]).wait()

    for j in range(8):
        flat[:, j * 128 : (j + 1) * 128] = placed[j].reshape(128, 128)
    skeleton = flat[:, 768:].astype(F32) - dot(flat[...], whole[...])
    s_one[core] = skeleton.astype(BF)

    c = remote(s_one.at[core], s_one.at[core], s_sem.at[0, 0], s_sem.at[1, 0], twin)
    c.start()
    projected = dot(flat[...], basis[...]).astype(BF)
    middle = dot(projected, inner[...]).astype(BF)
    correction = lax.dot_general(
        middle, basis[:768], (((1,), (1,)), ((), ())), preferred_element_type=F32
    )
    leading[...] = (flat[:, :768].astype(F32) - correction).astype(BF)
    pieces[3].wait_recv()
    local[0].wait()
    c.wait_recv()
    pieces.append(c)
    joined = dot(s_one[0], w_one[0]) + dot(s_one[1], w_one[1])
    s_two[in_quad] = joined[:, 128:].astype(BF)

    arriving = []
    for d in range(1, 4):
        c = remote(
            s_two.at[in_quad],
            s_two.at[in_quad],
            s_sem.at[0, d],
            s_sem.at[1, d],
            quad + lax.rem(in_quad + d, 4),
        )
        c.start()
        arriving.append(c)
    first_out[...] = joined[:, :128]
    leaf_out[...] = dot(leading[...], inverse[...]).astype(BF)
    for c in pieces[4:7]:
        c.wait_recv()
    local[1].wait()
    for c in arriving:
        c.wait_recv()
    pieces += arriving
    joined = dot(s_two[0], w_two[0])
    for i in range(1, 4):
        joined += dot(s_two[i], w_two[i])
    low = lax.broadcasted_iota(jnp.int32, (64, 128), 1) < 64
    s_three[in_group] = jnp.where(low, pltpu.roll(joined[:64], 64, 1), joined[64:]).astype(BF)

    arriving = []
    for d in range(1, GROUP):
        c = remote(
            s_three.at[in_group],
            s_three.at[in_group],
            s_sem.at[0, 3 + d],
            s_sem.at[1, 3 + d],
            group + lax.rem(in_group + d, GROUP),
        )
        c.start()
        arriving.append(c)
    second_out[...] = joined.T[:64]
    for c in pieces[7:14]:
        c.wait_recv()
    local[2].wait()
    odd = in_group % 2 == 1
    for i in range(GROUP):
        w = w_three[i].astype(F32)
        turned = pltpu.roll(w, 64, 1)
        w_wide[i, :64] = jnp.where(low, jnp.where(odd, turned, w), 0.0).astype(BF)
        w_wide[i, 64:] = jnp.where(low, 0.0, jnp.where(odd, w, turned)).astype(BF)
    for c in arriving:
        c.wait_recv()
    pieces += arriving
    joined = dot(s_three[0], w_wide[0])
    for i in range(1, GROUP):
        joined += dot(s_three[i], w_wide[i])
    turned = joined.T
    last_out[:, :64] = turned[:64]
    last_out[:, 64:] = turned[64:]

    pltpu.make_async_copy(half, half, twin_sem.at[0]).wait()
    part = pool.at[pl.ds(0, (CHIPS - 1) * 8)]
    pltpu.make_async_copy(part, part, spread_sem.at[8]).wait()
    part = picked.at[pl.ds(0, CHIPS - 1)]
    pltpu.make_async_copy(part, part, gather_sem.at[0]).wait()
    for c in pieces:
        c.wait_send()


def finish(leaf_in, first_in, second_in, last_in, leaf, first, second, third, top):
    leaf[...] = leaf_in[...]
    first[...] = first_in[...]
    second[...] = second_in[...]
    third[...] = last_in[:32]
    top[...] = last_in[32:]


def shards(right_sides, block_order, basis, inner, inverse, coupling, one, two, three):
    rows = right_sides.reshape(16, 4, 2, 8, 128).transpose(0, 3, 1, 2, 4)
    anywhere = pl.BlockSpec(memory_space=pl.ANY)
    vmem = pl.BlockSpec(memory_space=pltpu.VMEM)
    results = pl.pallas_call(
        kernel,
        out_shape=(
            jax.ShapeDtypeStruct((128, 768), BF),
            jax.ShapeDtypeStruct((128, 128), F32),
            jax.ShapeDtypeStruct((64, 128), F32),
            jax.ShapeDtypeStruct((64, 128), F32),
        ),
        in_specs=[anywhere] * 9,
        out_specs=(vmem,) * 4,
        scratch_shapes=[
            pltpu.SMEM((1024,), jnp.int32),
            pltpu.VMEM((16, 8, 4, 2, 128), BF),
            pltpu.VMEM((1024, 2, 128), BF),
            pltpu.VMEM((CHIPS, 8, 2, 128), BF),
            pltpu.VMEM((8, CHIPS, 2, 128), BF),
            pltpu.VMEM((128, 1024), BF),
            pltpu.VMEM((1024, 256), BF),
            pltpu.VMEM((256, 256), BF),
            pltpu.VMEM((768, 768), BF),
            pltpu.VMEM((768, 256), BF),
            pltpu.VMEM((1024, 256), BF),
            pltpu.VMEM((128, 768), BF),
            pltpu.VMEM((256, 512), BF),
            pltpu.VMEM((128, 512), BF),
            pltpu.VMEM((64, 512), BF),
            pltpu.VMEM((2, 256, 256), BF),
            pltpu.VMEM((4, 128, 128), BF),
            pltpu.VMEM((GROUP, 64, 128), BF),
            pltpu.VMEM((GROUP, 128, 128), BF),
            pltpu.VMEM((2, 128, 256), BF),
            pltpu.VMEM((4, 128, 128), BF),
            pltpu.VMEM((GROUP, 64, 128), BF),
            pltpu.SemaphoreType.DMA((9,)),
            pltpu.SemaphoreType.DMA((4,)),
            pltpu.SemaphoreType.DMA((9,)),
            pltpu.SemaphoreType.DMA((2,)),
            pltpu.SemaphoreType.DMA((2,)),
            pltpu.SemaphoreType.DMA((2, 4)),
            pltpu.SemaphoreType.DMA((2, 11)),
            pltpu.SemaphoreType.DMA((2, 11)),
        ],
        compiler_params=pltpu.CompilerParams(collective_id=0, has_side_effects=True),
    )(block_order, rows, basis[0], inner[0], inverse[0], coupling[0], one, two, three)
    leaf, first, second, third, top = pl.pallas_call(
        finish,
        out_shape=(
            jax.ShapeDtypeStruct((128, 768), BF),
            jax.ShapeDtypeStruct((128, 128), F32),
            jax.ShapeDtypeStruct((64, 128), F32),
            jax.ShapeDtypeStruct((32, 128), F32),
            jax.ShapeDtypeStruct((32, 128), F32),
        ),
        in_specs=[vmem] * 4,
        out_specs=(vmem,) * 5,
    )(*results)
    return leaf, first, second.T, third.T, top.T


def solution(mesh):
    return jax.shard_map(
        shards,
        mesh=mesh,
        in_specs=(
            P("rhs", "leaf"),
            P(),
            P("leaf", None, None),
            P("leaf", None, None),
            P("leaf", "rhs", None),
            P("leaf", None, None),
            P("leaf", None),
            P("leaf", None),
            P("leaf", None),
        ),
        out_specs=(P("rhs", "leaf"),) * 5,
        check_vma=False,
    )
```

```python
import jax
import jax.numpy as jnp
from jax import lax
from jax.experimental import pallas as pl
from jax.experimental.pallas import tpu as pltpu
from jax.sharding import PartitionSpec as P

BF = jnp.bfloat16
F32 = jnp.float32
CHIPS = 64
GROUP = 8
PLANES = 4
STEPS = (4, 3, 5, 2, 6, 1, 7, 0)


def dot(a, b):
    return jnp.dot(a, b, preferred_element_type=F32)


def kernel(
    order_in,
    rows_in,
    basis_in,
    inner_in,
    inverse_in,
    coupling_in,
    one_in,
    two_in,
    three_in,
    leaf_out,
    first_out,
    second_out,
    last_out,
    order,
    rows,
    pool,
    picked,
    placed,
    flat,
    basis,
    inner,
    inverse,
    coupling,
    whole,
    leading,
    one,
    two,
    three,
    w_one,
    w_two,
    w_three,
    w_wide,
    s_one,
    s_two,
    s_three,
    load_sem,
    own_sem,
    spread_sem,
    twin_sem,
    gather_sem,
    inv_sem,
    w_sem,
    s_sem,
):
    me = lax.axis_index("leaf")
    plane = lax.axis_index("rhs")
    chip = me // 2
    core = me % 2
    in_group = me % GROUP
    group = me - in_group
    in_quad = me % 4
    quad = me - in_quad
    twin = me + 1 - 2 * core
    row, column = chip // 8, chip % 8

    def remote(src, dst, send, recv, target, axis="leaf"):
        return pltpu.make_async_remote_copy(
            src_ref=src,
            dst_ref=dst,
            send_sem=send,
            recv_sem=recv,
            device_id={axis: target},
            device_id_type=pl.DeviceIdType.MESH,
        )

    def step(i):
        far = (8 - i) // 2
        return far + (1 - i % 2) * (1 - i // 7) * lax.rem(8 - 2 * far, 8)

    columns = [lax.rem(column + STEPS[j], 8) for j in range(8)]

    def each_chip(visit):
        def one_row(i, _):
            first = lax.rem(row + step(i), 8) * 8
            for j in range(8):
                visit(first + columns[j], i)
            return 0

        lax.fori_loop(0, 7, one_row, 0)
        for j in range(7):
            visit(row * 8 + columns[j], 7)

    barrier = pltpu.get_barrier_semaphore()

    def greet(target, axis="leaf"):
        pl.semaphore_signal(
            barrier, inc=1, device_id={axis: target}, device_id_type=pl.DeviceIdType.MESH
        )

    each_chip(lambda other, i: greet(other * 2 + core))
    for i in range(GROUP // 2):
        greet(group + 2 * i + 1 - core)
    for d in range(1, PLANES):
        greet(lax.rem(plane + d, PLANES), "rhs")
    loads = [
        (rows_in, rows),
        (inverse_in, inverse.at[pl.ds(pl.multiple_of(plane * 192, 64), 192)]),
        (one_in, one),
        (two_in, two),
        (three_in, three),
        (basis_in, basis),
        (inner_in, inner),
        (coupling_in, coupling),
        (order_in, order),
    ]
    loads = [pltpu.make_async_copy(a, b, load_sem.at[i]) for i, (a, b) in enumerate(loads)]
    for load in loads:
        load.start()
    pl.semaphore_wait(barrier, CHIPS - 1 + GROUP // 2 + PLANES - 1)

    loads[0].wait()
    mine = pl.ds(pl.multiple_of(me * 8, 8), 8)

    def spread(other, i):
        remote(
            rows.at[other // 4, :, other % 4],
            pool.at[mine],
            spread_sem.at[8],
            spread_sem.at[i],
            other * 2 + core,
        ).start()

    each_chip(spread)
    own = pltpu.make_async_copy(rows.at[chip // 4, :, chip % 4], pool.at[mine], own_sem.at[0])
    own.start()

    pieces = []
    loads[1].wait()
    for d in range(1, PLANES):
        share = inverse.at[pl.ds(pl.multiple_of(plane * 192, 64), 192)]
        c = remote(
            share, share, inv_sem.at[0, d], inv_sem.at[1, d], lax.rem(plane + d, PLANES), "rhs"
        )
        c.start()
        pieces.append(c)
    def hand(i, count):
        part = pool.at[pl.ds(0, count * 8)]
        pltpu.make_async_copy(part, part, spread_sem.at[i]).wait()
        origin = lax.rem(row + 8 - step(i), 8)

        def one_leaf(y, _):
            block = pool.at[pl.ds(pl.multiple_of(((origin * 8 + y) * 2 + core) * 8, 8), 8)]
            remote(block, block, twin_sem.at[0], twin_sem.at[1], twin).start()
            return 0

        lax.fori_loop(0, 8, one_leaf, 0)
        return 0

    lax.fori_loop(0, 7, lambda i, _: hand(i, 8), 0)
    own.wait()
    hand(7, 7)
    loads[8].wait()
    half = pool.at[pl.ds(0, CHIPS * 8)]
    pltpu.make_async_copy(half, half, twin_sem.at[1]).wait()

    def send(other):
        remote(
            picked.at[other],
            placed.at[:, chip],
            gather_sem.at[0],
            gather_sem.at[1],
            other * 2 + core,
        ).start()

    def pick(other):
        first = (other * 2 + core) * 8
        blocks = [pool[order[first + j]] for j in range(8)]
        for j in range(8):
            picked[other, j] = blocks[j]

    def gather(i, _):
        first = lax.rem(row + step(i), 8) * 8
        for j in range(8):
            pick(first + columns[j])
            if j > 0:
                send(first + columns[j - 1])
        send(first + columns[7])
        return 0

    lax.fori_loop(0, 7, gather, 0)
    for j in range(8):
        pick(row * 8 + columns[j])
        if j > 0:
            send(row * 8 + columns[j - 1])
    own = pltpu.make_async_copy(picked.at[chip], placed.at[:, chip], own_sem.at[0])
    own.start()
    for load in loads[2:5]:
        load.wait()
    c = remote(
        one.at[:, pl.ds(pl.multiple_of((1 - core) * 256, 256), 256)],
        w_one.at[core],
        w_sem.at[0, 0],
        w_sem.at[1, 0],
        twin,
    )
    c.start()
    pieces.append(c)
    local = [
        pltpu.make_async_copy(
            one.at[:, pl.ds(pl.multiple_of(core * 256, 256), 256)], w_one.at[core], own_sem.at[1]
        ),
        pltpu.make_async_copy(
            two.at[:, pl.ds(pl.multiple_of(in_quad * 128, 128), 128)],
            w_two.at[in_quad],
            own_sem.at[2],
        ),
        pltpu.make_async_copy(
            three.at[:, pl.ds(pl.multiple_of(in_group // 2 * 128, 128), 128)],
            w_three.at[in_group],
            own_sem.at[3],
        ),
    ]
    for c in local:
        c.start()
    for d in range(1, 4):
        other = lax.rem(in_quad + d, 4)
        c = remote(
            two.at[:, pl.ds(pl.multiple_of(other * 128, 128), 128)],
            w_two.at[in_quad],
            w_sem.at[0, d],
            w_sem.at[1, d],
            quad + other,
        )
        c.start()
        pieces.append(c)
    for d in range(1, GROUP):
        other = lax.rem(in_group + d, GROUP)
        c = remote(
            three.at[:, pl.ds(pl.multiple_of(other // 2 * 128, 128), 128)],
            w_three.at[in_group],
            w_sem.at[0, 3 + d],
            w_sem.at[1, 3 + d],
            group + other,
        )
        c.start()
        pieces.append(c)
    for load in loads[5:8]:
        load.wait()
    own.wait()

    spread_back = lax.dot_general(
        inner[...], basis[...], (((1,), (1,)), ((), ())), preferred_element_type=F32
    )
    for c in pieces[:3]:
        c.wait_recv()
    folded = dot(inverse[...], coupling[...])
    folded_low = folded.astype(BF)
    rest = spread_back[:, 768:] - dot(spread_back[:, :768].astype(BF), folded_low)
    rest = rest.astype(BF)
    whole[:768] = (folded + dot(basis[:768], rest)).astype(BF)
    whole[768:] = dot(basis[768:], rest).astype(BF)

    part = picked.at[pl.ds(0, CHIPS - 1)]
    pltpu.make_async_copy(part, part, gather_sem.at[1]).wait()

    for j in range(8):
        flat[:, j * 128 : (j + 1) * 128] = placed[j].reshape(128, 128)
    skeleton = flat[:, 768:].astype(F32) - dot(flat[...], whole[...])
    s_one[core] = skeleton.astype(BF)

    c = remote(s_one.at[core], s_one.at[core], s_sem.at[0, 0], s_sem.at[1, 0], twin)
    c.start()
    projected = dot(flat[...], basis[...]).astype(BF)
    middle = dot(projected, inner[...]).astype(BF)
    correction = lax.dot_general(
        middle, basis[:768], (((1,), (1,)), ((), ())), preferred_element_type=F32
    )
    leading[...] = (flat[:, :768].astype(F32) - correction).astype(BF)
    pieces[3].wait_recv()
    local[0].wait()
    c.wait_recv()
    pieces.append(c)
    joined = dot(s_one[0], w_one[0]) + dot(s_one[1], w_one[1])
    s_two[in_quad] = joined[:, 128:].astype(BF)

    arriving = []
    for d in range(1, 4):
        c = remote(
            s_two.at[in_quad],
            s_two.at[in_quad],
            s_sem.at[0, d],
            s_sem.at[1, d],
            quad + lax.rem(in_quad + d, 4),
        )
        c.start()
        arriving.append(c)
    first_out[...] = joined[:, :128]
    leaf_out[...] = dot(leading[...], inverse[...]).astype(BF)
    for c in pieces[4:7]:
        c.wait_recv()
    local[1].wait()
    for c in arriving:
        c.wait_recv()
    pieces += arriving
    joined = dot(s_two[0], w_two[0])
    for i in range(1, 4):
        joined += dot(s_two[i], w_two[i])
    low = lax.broadcasted_iota(jnp.int32, (64, 128), 1) < 64
    s_three[in_group] = jnp.where(low, pltpu.roll(joined[:64], 64, 1), joined[64:]).astype(BF)

    arriving = []
    for d in range(1, GROUP):
        c = remote(
            s_three.at[in_group],
            s_three.at[in_group],
            s_sem.at[0, 3 + d],
            s_sem.at[1, 3 + d],
            group + lax.rem(in_group + d, GROUP),
        )
        c.start()
        arriving.append(c)
    second_out[...] = joined.T[:64]
    for c in pieces[7:14]:
        c.wait_recv()
    local[2].wait()
    odd = in_group % 2 == 1
    for i in range(GROUP):
        w = w_three[i].astype(F32)
        turned = pltpu.roll(w, 64, 1)
        w_wide[i, :64] = jnp.where(low, jnp.where(odd, turned, w), 0.0).astype(BF)
        w_wide[i, 64:] = jnp.where(low, 0.0, jnp.where(odd, w, turned)).astype(BF)
    for c in arriving:
        c.wait_recv()
    pieces += arriving
    joined = dot(s_three[0], w_wide[0])
    for i in range(1, GROUP):
        joined += dot(s_three[i], w_wide[i])
    turned = joined.T
    last_out[:, :64] = turned[:64]
    last_out[:, 64:] = turned[64:]

    pltpu.make_async_copy(half, half, twin_sem.at[0]).wait()
    part = pool.at[pl.ds(0, (CHIPS - 1) * 8)]
    pltpu.make_async_copy(part, part, spread_sem.at[8]).wait()
    part = picked.at[pl.ds(0, CHIPS - 1)]
    pltpu.make_async_copy(part, part, gather_sem.at[0]).wait()
    for c in pieces:
        c.wait_send()


def finish(leaf_in, first_in, second_in, last_in, leaf, first, second, third, top):
    leaf[...] = leaf_in[...]
    first[...] = first_in[...]
    second[...] = second_in[...]
    third[...] = last_in[:32]
    top[...] = last_in[32:]


def shards(right_sides, block_order, basis, inner, inverse, coupling, one, two, three):
    rows = right_sides.reshape(16, 4, 2, 8, 128).transpose(0, 3, 1, 2, 4)
    anywhere = pl.BlockSpec(memory_space=pl.ANY)
    vmem = pl.BlockSpec(memory_space=pltpu.VMEM)
    results = pl.pallas_call(
        kernel,
        out_shape=(
            jax.ShapeDtypeStruct((128, 768), BF),
            jax.ShapeDtypeStruct((128, 128), F32),
            jax.ShapeDtypeStruct((64, 128), F32),
            jax.ShapeDtypeStruct((64, 128), F32),
        ),
        in_specs=[anywhere] * 9,
        out_specs=(vmem,) * 4,
        scratch_shapes=[
            pltpu.SMEM((1024,), jnp.int32),
            pltpu.VMEM((16, 8, 4, 2, 128), BF),
            pltpu.VMEM((1024, 2, 128), BF),
            pltpu.VMEM((CHIPS, 8, 2, 128), BF),
            pltpu.VMEM((8, CHIPS, 2, 128), BF),
            pltpu.VMEM((128, 1024), BF),
            pltpu.VMEM((1024, 256), BF),
            pltpu.VMEM((256, 256), BF),
            pltpu.VMEM((768, 768), BF),
            pltpu.VMEM((768, 256), BF),
            pltpu.VMEM((1024, 256), BF),
            pltpu.VMEM((128, 768), BF),
            pltpu.VMEM((256, 512), BF),
            pltpu.VMEM((128, 512), BF),
            pltpu.VMEM((64, 512), BF),
            pltpu.VMEM((2, 256, 256), BF),
            pltpu.VMEM((4, 128, 128), BF),
            pltpu.VMEM((GROUP, 64, 128), BF),
            pltpu.VMEM((GROUP, 128, 128), BF),
            pltpu.VMEM((2, 128, 256), BF),
            pltpu.VMEM((4, 128, 128), BF),
            pltpu.VMEM((GROUP, 64, 128), BF),
            pltpu.SemaphoreType.DMA((9,)),
            pltpu.SemaphoreType.DMA((4,)),
            pltpu.SemaphoreType.DMA((9,)),
            pltpu.SemaphoreType.DMA((2,)),
            pltpu.SemaphoreType.DMA((2,)),
            pltpu.SemaphoreType.DMA((2, 4)),
            pltpu.SemaphoreType.DMA((2, 11)),
            pltpu.SemaphoreType.DMA((2, 11)),
        ],
        compiler_params=pltpu.CompilerParams(collective_id=0, has_side_effects=True),
    )(block_order, rows, basis[0], inner[0], inverse[0], coupling[0], one, two, three)
    leaf, first, second, third, top = pl.pallas_call(
        finish,
        out_shape=(
            jax.ShapeDtypeStruct((128, 768), BF),
            jax.ShapeDtypeStruct((128, 128), F32),
            jax.ShapeDtypeStruct((64, 128), F32),
            jax.ShapeDtypeStruct((32, 128), F32),
            jax.ShapeDtypeStruct((32, 128), F32),
        ),
        in_specs=[vmem] * 4,
        out_specs=(vmem,) * 5,
    )(*results)
    return leaf, first, second.T, third.T, top.T


def solution(mesh):
    return jax.shard_map(
        shards,
        mesh=mesh,
        in_specs=(
            P("rhs", "leaf"),
            P(),
            P("leaf", None, None),
            P("leaf", None, None),
            P("leaf", "rhs", None),
            P("leaf", None, None),
            P("leaf", None),
            P("leaf", None),
            P("leaf", None),
        ),
        out_specs=(P("rhs", "leaf"),) * 5,
        check_vma=False,
    )
```
